32 devices in a mesh: groups: 2 (over y), tm: 4 (over z), chan: 4 (over x, core).
Axes of the slice: x: 2, y: 2, z: 4, core: 2. Of those that a mesh axis runs over, the one named last changes fastest.
Arguments:
- tokens: bfloat16 [1024, 4096], P(('groups', 'tm'), 'chan'), parts along dimension 0, may hold values from -6 to 6
- in_weight: bfloat16 [4096, 8192], P('chan'), may hold values from -0.125 to 0.125
- recur_weight: float32 [2048, 2], P('chan'), may hold values from -0.75 to 0.75
- gate_bias: float32 [2048, 4], P('chan'), may hold values from -2 to 13
- forget_offset: float32 [1024], P(('groups', 'tm')), parts along dimension 0, may hold values from 0 to 14
Outputs:
- hidden_states: float32 [2048, 1024], P('chan', ('groups', 'tm')), parts along dimension 1
The draws below stay inside these ranges and needn't reach their ends.
There are 2 independent parts, one for each index of `groups`. The reference program is written for one: setup_inputs(seed, part) draws one part's arguments, and reference() takes and returns one part's arrays. A program takes and returns all parts, laid end to end along the dimension named above; an argument that names none is the same for every part. Nothing has to cross between parts.
All inputs are finite; a program needn't handle non-finite values.
Results may differ from the reference program's by a relative error of at most 0.0003.
Values may be sent and summed in bfloat16 or wider, within the bound.
A program may use at most 128 MiB of HBM per device.

```python
import math
import jax
import jax.numpy as jnp
from jax import lax

D = 4096
H = 2048
ITERS = 2
TOKENS = 512


def draw_gate_bias(key, part):
    keys = jax.random.split(jax.random.fold_in(key, 11), 3)
    others = jnp.clip(jax.random.normal(keys[0], (H, 4), jnp.float32) * 0.7, -2.0, 2.0)
    slow_share = 0.5
    slow = jax.random.uniform(keys[1], (H,), jnp.float32) < slow_share
    position = jax.random.uniform(keys[2], (H,), jnp.float32)
    lowest = math.log(30.0)
    middle = math.log(2.0 * TOKENS)
    highest = math.log(32.0 * TOKENS)
    forget = jnp.where(slow, middle + position * (highest - middle), lowest + position * (middle - lowest))
    return others.at[:, 1].set(forget)


def draw_forget_offset(key, part):
    keys = jax.random.split(jax.random.fold_in(key, 23), 2)
    spots = jax.random.randint(keys[0], (6,), 0, TOKENS)
    values = jax.random.uniform(keys[1], (6,), jnp.float32, 10.0, 14.0)
    return jnp.zeros((TOKENS,), jnp.float32).at[spots].set(values)


def strengthened(array, stream_key, source, target, shards_of, factor):
    owner, partner = [(jnp.arange(array.shape[dim]) // (array.shape[dim] // shards_of)).reshape([-1 if axis == dim else 1 for axis in range(array.ndim)]) for dim in (source, target)]
    chosen = jax.random.permutation(stream_key, shards_of)[partner]
    strong = (owner == chosen) | (owner == (partner + shards_of // 2) % shards_of)
    return jnp.where(strong, factor * array, array)


def levels(stream_key, shape, pieces, least, high):
    def one(dim, blocks):
        draws = jax.random.uniform(jax.random.fold_in(jax.random.fold_in(stream_key, 6), dim), (blocks,), jnp.float32, least / len(pieces), high / len(pieces))
        return jnp.repeat(jnp.exp(draws), shape[dim] // blocks).reshape((-1,) + (1,) * (len(shape) - dim - 1))

    level = one(*pieces[0])
    for cut in pieces[1:]:
        level = level * one(*cut)
    return level


def noise(key, shape, deviation, reach, cuts=(), held_as=jnp.bfloat16):
    entries = deviation * jax.random.normal(key, shape, jnp.float32)
    if cuts:
        entries = entries * levels(key, shape, cuts, -0.22, 0.18)
    return jnp.clip(entries, -reach, reach).astype(held_as)


def gaussian_with(stream_key, dims, spread, most, pieces, heavy, held_as=jnp.bfloat16):
    drawn = spread * jax.random.normal(stream_key, dims, jnp.float32)
    if pieces:
        drawn = drawn * levels(stream_key, dims, pieces, -0.22, 0.18)
    return jnp.clip(strengthened(drawn, jax.random.fold_in(stream_key, 3), *heavy), -most, most).astype(held_as)


def setup_inputs(seed: int = 0, part: int = 0) -> dict:
    seeds = jax.random.split(jax.random.key(seed), 6)
    part_keys = jax.random.split(jax.random.fold_in(seeds[5], part), 6)
    tokens = noise(part_keys[0], (TOKENS, D), 1.0, 6.0, ((0, 4), (1, 4)))
    in_weight = gaussian_with(seeds[1], (D, 4 * H), D ** -0.5, 0.125, ((0, 4),), (0, 1, 4, 2.0))
    recur_weight = jnp.clip(jax.random.uniform(seeds[2], (H, 2), jnp.float32, -0.75, 0.75) * levels(seeds[2], (H, 2), ((0, 4),), -0.4, 0.0), -0.75, 0.75)
    gate_bias = draw_gate_bias(jax.random.fold_in(seeds[5], 71), part)
    forget_offset = draw_forget_offset(jax.random.fold_in(jax.random.fold_in(seeds[5], part), 71), part)
    return dict(tokens=tokens, in_weight=in_weight, recur_weight=recur_weight, gate_bias=gate_bias, forget_offset=forget_offset)


def gates(projected, prev_cell, prev_hidden, gate_bias, recur_weight, forget_offset):
    input_gate = jax.nn.sigmoid(projected[:, 0] + gate_bias[:, 0:1])
    forget_gate = jax.nn.sigmoid(projected[:, 1] + gate_bias[:, 1:2] + recur_weight[:, 0:1] * prev_hidden - forget_offset[None, :])
    cand_gate = jnp.tanh(projected[:, 2] + gate_bias[:, 2:3])
    output_gate = jax.nn.sigmoid(projected[:, 3] + gate_bias[:, 3:4] + recur_weight[:, 1:2] * prev_hidden)
    new_cell = forget_gate * prev_cell + input_gate * cand_gate
    squashed = jnp.tanh(new_cell)
    new_hidden = output_gate * squashed
    slope = 1.0 - squashed * squashed
    cell_cell = forget_gate
    cell_hidden = prev_cell * forget_gate * (1.0 - forget_gate) * recur_weight[:, 0:1]
    hidden_cell = output_gate * slope * forget_gate
    hidden_hidden = output_gate * (1.0 - output_gate) * recur_weight[:, 1:2] * squashed + output_gate * slope * cell_hidden
    offset_cell = new_cell - cell_cell * prev_cell - cell_hidden * prev_hidden
    offset_hidden = new_hidden - hidden_cell * prev_cell - hidden_hidden * prev_hidden
    return (cell_cell, cell_hidden, hidden_cell, hidden_hidden, offset_cell, offset_hidden)


def advance(carry, term):
    cell, hidden = carry
    new_cell = term[0] * cell + term[1] * hidden + term[4]
    new_hidden = term[2] * cell + term[3] * hidden + term[5]
    return (new_cell, new_hidden), (new_cell, new_hidden)


def reference(tokens, in_weight, recur_weight, gate_bias, forget_offset):
    projected = jnp.dot(tokens, in_weight, preferred_element_type=jnp.float32)
    projected = projected.reshape(TOKENS, H, 4).transpose(1, 2, 0)
    prev_cell = jnp.zeros((H, TOKENS), jnp.float32)
    prev_hidden = jnp.zeros((H, TOKENS), jnp.float32)
    hiddens = prev_hidden
    for repeat in range(ITERS):
        terms = gates(projected, prev_cell, prev_hidden, gate_bias, recur_weight, forget_offset)
        stacked = jnp.stack(terms).transpose(2, 0, 1)
        start_state = (jnp.zeros((H,), jnp.float32), jnp.zeros((H,), jnp.float32))
        final, (cells, hiddens) = lax.scan(advance, start_state, stacked)
        cells = cells.T
        hiddens = hiddens.T
        prev_cell = jnp.concatenate([jnp.zeros((H, 1), jnp.float32), cells[:, :-1]], axis=1)
        prev_hidden = jnp.concatenate([jnp.zeros((H, 1), jnp.float32), hiddens[:, :-1]], axis=1)
    return hiddens
```

```python
import functools
import math

import jax
import jax.numpy as jnp
from jax import lax
from jax.experimental import pallas as pl
from jax.experimental.pallas import tpu as pltpu
from jax.sharding import PartitionSpec as P

MESH = pl.DeviceIdType.MESH
LANES = 128
SUB = 8
GATES = 4
AHEAD = 6
PIECES = 2
LAG = 3
TOKEN_MOST = 6.0
WEIGHT_MOST = 0.125
KNEE = 8.0
SLOPE = 25.5
OCTAVES = 252.0
FLOOR = 126.0


def compose(early, later):
    e_one, e_two, e_three, e_four, e_five, e_six = early
    l_one, l_two, l_three, l_four, l_five, l_six = later
    return (
        l_one * e_one + l_two * e_three,
        l_one * e_two + l_two * e_four,
        l_three * e_one + l_four * e_three,
        l_three * e_two + l_four * e_four,
        l_one * e_five + l_two * e_six + l_five,
        l_three * e_five + l_four * e_six + l_six,
    )


def compose_lower(early, later):
    e_one, e_three, e_four, e_five, e_six = early
    l_one, l_three, l_four, l_five, l_six = later
    return (
        l_one * e_one,
        l_three * e_one + l_four * e_three,
        l_four * e_four,
        l_one * e_five + l_five,
        l_three * e_five + l_four * e_six + l_six,
    )


def sigmoid(value):
    return 0.5 * jnp.tanh(0.5 * value) + 0.5


def knee_rate(most):
    return (OCTAVES - SLOPE * KNEE) / math.log(most / KNEE)


def encode(value, most):
    rate = knee_rate(most)
    size = jnp.abs(value)
    beyond = rate * jnp.log(jnp.maximum(size, KNEE)) + (SLOPE * KNEE - rate * math.log(KNEE))
    power = jnp.exp2(jnp.minimum(SLOPE * size, beyond) - FLOOR)
    return jnp.where(value < 0.0, -power, power).astype(jnp.bfloat16)


def decode(code, most):
    rate = knee_rate(most)
    level = jnp.log2(jnp.abs(code)) + FLOOR
    beyond = KNEE * jnp.exp((jnp.maximum(level, SLOPE * KNEE) - SLOPE * KNEE) * (1.0 / rate))
    size = jnp.where(level <= SLOPE * KNEE, level * (1.0 / SLOPE), beyond)
    return jnp.where(code < 0.0, -size, size)


def kernel(
    chips, blocks, tm, most,
    tokens_hbm, weight_hbm, recur_hbm, bias_hbm, offset_hbm, out_ref,
    tokens_v, sorted_v, weight_v, recur_v, bias_v, offset_v,
    part_v, take_v, far_out, far_in, unmix, code_v,
    turned, near_v, pre_v, input_v, prefix_v, edge_v, maps_v, hidden_v,
    tokens_sem, small_sem, weight_sem, give_send, give_recv, far_send, far_recv, map_send, map_recv,
    ready_sem,
):
    my_chan = lax.axis_index("chan")
    my_tm = lax.axis_index("tm")
    chip = my_chan // 2
    core = my_chan % 2
    partner = chip * 2 + (1 - core)
    held = blocks * PIECES
    units = chips * held
    far = units - held
    width = GATES * LANES
    thin = width // PIECES
    steps = tokens_v.shape[0]
    run = steps // SUB

    def chip_of(rank):
        return lax.rem(chip + rank + 1, chips)

    def place(index):
        near = jnp.where(index >= 2 * far, 1, 0)
        local = index - near * 2 * far
        count = jnp.where(near == 1, held, far)
        late = jnp.where(local >= count, 1, 0)
        return late, near * far + local - late * count

    def weight_copy(index):
        owner, unit = place(index)
        target = chip_of(unit // held) * 2 + owner
        column = pl.multiple_of((target * held + unit % held) * thin, thin)
        return pltpu.make_async_copy(
            weight_hbm.at[:, pl.ds(column, thin)], weight_v.at[index], weight_sem.at[index]
        )

    def give_copy(unit):
        return pltpu.make_async_remote_copy(
            src_ref=part_v.at[unit, 1 - core],
            dst_ref=take_v.at[unit],
            send_sem=give_send.at[unit],
            recv_sem=give_recv.at[unit],
            device_id={"chan": partner},
            device_id_type=MESH,
        )

    def far_copy(unit):
        return pltpu.make_async_remote_copy(
            src_ref=far_out.at[unit],
            dst_ref=far_in.at[unit],
            send_sem=far_send.at[unit],
            recv_sem=far_recv.at[unit],
            device_id={"chan": chip_of(unit // held) * 2 + core},
            device_id_type=MESH,
        )

    def map_copy(turn, block, source, target):
        slot = (turn * blocks + block) * tm + source
        return pltpu.make_async_remote_copy(
            src_ref=maps_v.at[slot],
            dst_ref=maps_v.at[slot],
            send_sem=map_send.at[(turn * blocks + block) * tm + target],
            recv_sem=map_recv.at[slot],
            device_id={"tm": target},
            device_id_type=MESH,
        )

    tokens_copy = pltpu.make_async_copy(tokens_hbm, tokens_v, tokens_sem)
    tokens_copy.start()
    for index in range(AHEAD):
        weight_copy(index).start()

    barrier = pltpu.get_barrier_semaphore()
    pl.semaphore_signal(barrier, inc=1, device_id={"chan": partner}, device_id_type=MESH)
    for rank in range(chips - 1):
        pl.semaphore_signal(
            barrier, inc=1, device_id={"chan": chip_of(rank) * 2 + core}, device_id_type=MESH
        )

    def greet(peer, carry):
        pl.semaphore_signal(barrier, inc=1, device_id={"tm": peer}, device_id_type=MESH)
        return carry

    lax.fori_loop(my_tm + 1, tm, greet, 0)

    small = [
        pltpu.make_async_copy(held, local, small_sem.at[index])
        for index, (held, local) in enumerate(
            ((recur_hbm, recur_v), (bias_hbm, bias_v), (offset_hbm, offset_v))
        )
    ]
    for copy in small:
        copy.start()

    row = lax.broadcasted_iota(jnp.int32, (steps, steps), 0)
    column = lax.broadcasted_iota(jnp.int32, (steps, steps), 1)
    sort = jnp.where(column == (row % SUB) * run + row // SUB, 1.0, 0.0).astype(tokens_v.dtype)
    row = lax.broadcasted_iota(jnp.int32, (width, width), 0)
    column = lax.broadcasted_iota(jnp.int32, (width, width), 1)
    wanted = (column % LANES) * GATES + column // LANES
    unmix[...] = jnp.where(row == wanted, 1.0, 0.0).astype(jnp.bfloat16)

    tokens_copy.wait()
    sorted_v[...] = jnp.dot(sort, tokens_v[...], preferred_element_type=jnp.float32).astype(
        sorted_v.dtype
    )
    pl.semaphore_wait(barrier, chips + my_tm)

    def answer(peer, carry):
        pl.semaphore_signal(ready_sem, inc=1, device_id={"tm": peer}, device_id_type=MESH)
        return carry

    lax.fori_loop(0, my_tm, answer, 0)

    def product(index):
        weight_copy(index).wait()

        @pl.when(index + AHEAD < 2 * units)
        def _():
            weight_copy(index + AHEAD).start()

        return jnp.dot(sorted_v[...], weight_v[index], preferred_element_type=jnp.float32)

    def forward(unit):
        give_copy(unit).wait_recv()
        far_out[unit] = encode(part_v[unit, core] + take_v[unit], most)
        far_copy(unit).start()

    def matmul_step(index, carry):
        owner, unit = place(index)
        part_v[unit, owner] = product(index)

        @pl.when(owner != core)
        def _():
            give_copy(unit).start()

        sent = index - core * far - LAG

        @pl.when((sent >= 0) & (sent < far))
        def _():
            forward(sent)

        return carry

    lax.fori_loop(0, 2 * units, matmul_step, 0)

    for copy in small:
        copy.wait()

    def near(block, carry):
        for piece in range(PIECES):
            unit = far + block * PIECES + piece
            give_copy(unit).wait_recv()
            total = part_v[unit, core] + take_v[unit]
            for tile in range(thin // LANES):
                lanes = slice(tile * LANES, (tile + 1) * LANES)
                turned[piece * thin + tile * LANES : piece * thin + (tile + 1) * LANES, :] = total[:, lanes].T
        rows = pl.ds(pl.multiple_of(block * LANES, LANES), LANES)
        for gate in range(GATES):
            value = turned[pl.ds(gate, LANES, stride=GATES), :].T
            near_v[block, gate] = value + bias_v[gate : gate + 1, rows]
        return carry

    lax.fori_loop(0, blocks, near, 0)
    wide = jnp.broadcast_to(offset_v[...], (LANES, steps)).T
    for step in range(run):
        hidden_v[step * SUB : (step + 1) * SUB] = wide[step * SUB : (step + 1) * SUB]
    for step in range(run):
        late = hidden_v[pl.ds(step, SUB, stride=run), :]
        for block in range(blocks):
            rows = slice(step * SUB, (step + 1) * SUB)
            near_v[block, 1, rows] = near_v[block, 1, rows] - late

    row_id = lax.broadcasted_iota(jnp.int32, (SUB, LANES), 0)

    def at(step):
        return slice(step * SUB, (step + 1) * SUB)

    def recur_rows(block):
        rows = pl.ds(pl.multiple_of(block * LANES, LANES), LANES)
        return [
            jnp.broadcast_to(recur_v[which : which + 1, rows], (SUB, LANES)) for which in range(2)
        ]

    def shifted(parts, by, identity):
        return tuple(
            jnp.where(row_id < by, unit_value, pltpu.roll(part, by, 0))
            for part, unit_value in zip(parts, identity)
        )

    lower_identity = (1.0, 0.0, 1.0, 0.0, 0.0)
    identity = (1.0, 0.0, 0.0, 1.0, 0.0, 0.0)

    def publish(turn, block, total, fold, neutral):
        for by in (1, 2, 4):
            total = fold(shifted(total, by, neutral), total)
        if len(total) == 5:
            total = (total[0], jnp.zeros_like(total[0])) + tuple(total[1:])
        slot = (turn * blocks + block) * tm + my_tm
        for part in range(6):
            maps_v[slot, part : part + 1, :] = total[part][SUB - 1 : SUB]
        maps_v[slot, 6:8, :] = jnp.zeros((2, LANES), jnp.float32)

        def send(back, carry):
            map_copy(turn, block, my_tm, tm - 1 - back).start()
            return carry

        lax.fori_loop(0, tm - 1 - my_tm, send, 0)
        before = shifted(total, 1, identity)
        for part in range(6):
            edge_v[turn, block, part] = before[part]

    def arriving(turn, block):
        def take(source, state):
            cell, hidden = state
            map_copy(turn, block, source, my_tm).wait_recv()
            held = maps_v[(turn * blocks + block) * tm + source]
            return (
                held[0:1] * cell + held[1:2] * hidden + held[4:5],
                held[2:3] * cell + held[3:4] * hidden + held[5:6],
            )

        zero = jnp.zeros((1, LANES), jnp.float32)
        cell, hidden = lax.fori_loop(0, my_tm, take, (zero, zero))
        edge = [edge_v[turn, block, part] for part in range(6)]
        return (
            edge[0] * cell + edge[1] * hidden + edge[4],
            edge[2] * cell + edge[3] * hidden + edge[5],
        )

    def first(block):
        for rank in range(chips - 1):
            code = jnp.zeros((steps, width), jnp.float32)
            for piece in range(PIECES):
                unit = rank * held + block * PIECES + piece
                far_copy(unit).wait_recv()
                code = code + jnp.dot(
                    far_in[unit],
                    unmix[piece * thin : (piece + 1) * thin, :],
                    preferred_element_type=jnp.float32,
                )
            for gate in range(GATES):
                code_v[rank, gate] = code[:, gate * LANES : (gate + 1) * LANES]
        _, recur_out = recur_rows(block)
        prefix = None
        for step in range(run):
            total = [near_v[block, gate, at(step)] for gate in range(GATES)]
            for rank in range(chips - 1):
                total = [
                    value + decode(code_v[rank, gate, at(step)], most)
                    for gate, value in enumerate(total)
                ]
            pre_v[block, 0, step] = total[1]
            pre_v[block, 1, step] = total[3]
            forget = sigmoid(total[1])
            output = sigmoid(total[3])
            fresh = sigmoid(total[0]) * jnp.tanh(total[2])
            squashed = jnp.tanh(fresh)
            slope = 1.0 - squashed * squashed
            input_v[block, step] = fresh
            term = (
                forget,
                output * slope * forget,
                output * (1.0 - output) * recur_out * squashed,
                fresh,
                output * squashed,
            )
            prefix = term if prefix is None else compose_lower(prefix, term)
            for part, value in enumerate(prefix):
                prefix_v[block, part, step] = value
        publish(0, block, prefix, compose_lower, lower_identity)

    def jacobian(block, step, cell, hidden, recur_forget, recur_out):
        forget = sigmoid(pre_v[block, 0, step] + recur_forget * hidden)
        output = sigmoid(pre_v[block, 1, step] + recur_out * hidden)
        fresh = input_v[block, step]
        squashed = jnp.tanh(forget * cell + fresh)
        slope = output * (1.0 - squashed * squashed)
        cell_hidden = cell * forget * (1.0 - forget) * recur_forget
        hidden_cell = slope * forget
        hidden_hidden = output * (1.0 - output) * recur_out * squashed + slope * cell_hidden
        return (
            forget,
            cell_hidden,
            hidden_cell,
            hidden_hidden,
            fresh - cell_hidden * hidden,
            output * squashed - hidden_cell * cell - hidden_hidden * hidden,
        )

    def second(block):
        start_cell, start_hidden = arriving(0, block)
        recur_forget, recur_out = recur_rows(block)
        cell, hidden = start_cell, start_hidden
        prefix = None
        for step in range(run):
            term = jacobian(block, step, cell, hidden, recur_forget, recur_out)
            if step + 1 < run:
                past = [prefix_v[block, part, step] for part in range(5)]
                cell = past[0] * start_cell + past[3]
                hidden = past[1] * start_cell + past[2] * start_hidden + past[4]
            prefix = term if prefix is None else compose(prefix, term)
            for part, value in ((0, prefix[2]), (1, prefix[3]), (2, prefix[5])):
                prefix_v[block, part + 5, step] = value
        publish(1, block, prefix, compose, identity)

    def third(block):
        start_cell, start_hidden = arriving(1, block)
        for step in range(run):
            past = [prefix_v[block, part + 5, step] for part in range(3)]
            hidden_v[pl.ds(step, SUB, stride=run), :] = (
                past[0] * start_cell + past[1] * start_hidden + past[2]
            )
        rows = pl.ds(pl.multiple_of(block * LANES, LANES), LANES)
        out_ref[rows, :] = hidden_v[...].T

    @pl.when(my_tm < tm - 1)
    def _():
        pl.semaphore_wait(ready_sem, tm - 1 - my_tm)

    def scan_step(turn, carry):
        @pl.when(turn < blocks)
        def _():
            first(turn)

        @pl.when((turn >= 1) & (turn <= blocks))
        def _():
            second(turn - 1)

        @pl.when(turn >= 2)
        def _():
            third(turn - 2)

        return carry

    lax.fori_loop(0, blocks + 2, scan_step, 0)

    def settle_units(unit, carry):
        give_copy(unit).wait_send()

        @pl.when(unit < far)
        def _():
            far_copy(unit).wait_send()

        return carry

    lax.fori_loop(0, units, settle_units, 0)

    def settle_maps(index, carry):
        def settle(target, carry):
            map_copy(index // blocks, index % blocks, my_tm, target).wait_send()
            return carry

        return lax.fori_loop(my_tm + 1, tm, settle, carry)

    lax.fori_loop(0, 2 * blocks, settle_maps, 0)


def shards(chan, tm, tokens, in_weight, recur_weight, gate_bias, forget_offset):
    steps, depth = tokens.shape
    channels = recur_weight.shape[0]
    chips = chan // 2
    blocks = channels // LANES
    held = blocks * PIECES
    units = chips * held
    far = max(1, units - held)
    width = GATES * LANES
    thin = width // PIECES
    run = steps // SUB
    most = max(2.0 * KNEE, 2 * depth * TOKEN_MOST * WEIGHT_MOST)
    hbm = pl.BlockSpec(memory_space=pltpu.HBM)
    dma = pltpu.SemaphoreType.DMA
    float32 = jnp.float32
    return pl.pallas_call(
        functools.partial(kernel, chips, blocks, tm, most),
        out_shape=pltpu.VMEM((channels, steps), float32),
        in_specs=[hbm] * 5,
        out_specs=pl.BlockSpec(memory_space=pltpu.VMEM),
        scratch_shapes=[
            pltpu.VMEM((steps, depth), tokens.dtype),
            pltpu.VMEM((steps, depth), tokens.dtype),
            pltpu.VMEM((2 * units, depth, thin), in_weight.dtype),
            pltpu.VMEM((2, channels), float32),
            pltpu.VMEM((GATES, channels), float32),
            pltpu.VMEM((1, steps), float32),
            pltpu.VMEM((units, 2, steps, thin), float32),
            pltpu.VMEM((units, steps, thin), float32),
            pltpu.VMEM((far, steps, thin), jnp.bfloat16),
            pltpu.VMEM((far, steps, thin), jnp.bfloat16),
            pltpu.VMEM((width, width), jnp.bfloat16),
            pltpu.VMEM((max(1, chips - 1), GATES, steps, LANES), float32),
            pltpu.VMEM((width, steps), float32),
            pltpu.VMEM((blocks, GATES, steps, LANES), float32),
            pltpu.VMEM((blocks, 2, run, SUB, LANES), float32),
            pltpu.VMEM((blocks, run, SUB, LANES), float32),
            pltpu.VMEM((blocks, 8, run, SUB, LANES), float32),
            pltpu.VMEM((2, blocks, 6, SUB, LANES), float32),
            pltpu.VMEM((2 * blocks * tm, SUB, LANES), float32),
            pltpu.VMEM((steps, LANES), float32),
            dma,
            dma((3,)),
            dma((2 * units,)),
            dma((units,)),
            dma((units,)),
            dma((far,)),
            dma((far,)),
            dma((2 * blocks * tm,)),
            dma((2 * blocks * tm,)),
            pltpu.SemaphoreType.REGULAR,
        ],
        compiler_params=pltpu.CompilerParams(
            collective_id=0, has_side_effects=True, vmem_limit_bytes=65000 * 1024
        ),
    )(tokens, in_weight, recur_weight.T, gate_bias.T, forget_offset.reshape(1, steps))


def solution(mesh):
    placed = (
        P(("groups", "tm"), "chan"),
        P("chan", None),
        P("chan", None),
        P("chan", None),
        P(("groups", "tm")),
    )
    return jax.shard_map(
        functools.partial(shards, mesh.shape["chan"], mesh.shape["tm"]),
        mesh=mesh,
        in_specs=placed,
        out_specs=P("chan", ("groups", "tm")),
        check_vma=False,
    )
```
